32 devices in a mesh: prow: 4 (over y, x), pcol: 8 (over z, core).
Axes of the slice: x: 2, y: 2, z: 4, core: 2. Of those that a mesh axis runs over, the one named last changes fastest.
Arguments:
- covariance: float32 [16384, 16384], P(('prow', 'pcol')), may hold values from -600 to 600, as said below
- factor_left: float32 [64, 16384], P(None, ('prow', 'pcol')), may hold values from -6 to 6
- factor_right: float32 [64, 16384], P('prow', 'pcol'), may hold values from -3 to 3
Outputs:
- whitened: float32 [16384, 16384], P('prow', 'pcol')
The draws below stay inside these ranges and needn't reach their ends.
Inputs may be any that keep to these rules, and one draw needn't show every extreme that they name: `covariance`: entries are real-valued and of full rank.
All inputs are finite; a program needn't handle non-finite values.
Results may differ from the reference program's by a relative error of at most 0.00007.
Values sent between devices are 32-bit elements; how exact they have to be, the bound alone decides.
A program may use at most 192 MiB of HBM per device.

```python
import jax
import jax.numpy as jnp
from jax import lax

ORDER = 16384
RANK = 64
TILE = 64
N_PROW = 4
N_PCOL = 8


def draw_covariance(key, part):
    subkeys = jax.random.split(key, 3)
    positions = jnp.arange(ORDER)
    tile_row = (positions // TILE % N_PROW).astype(jnp.float32)
    tile_col = (positions // TILE % N_PCOL).astype(jnp.float32)
    row_scale = jnp.exp(tile_row / (N_PROW - 1) * jnp.log(3.0) + jax.random.uniform(subkeys[0], (ORDER,)) * jnp.log(3.3))
    col_scale = jnp.exp(tile_col / (N_PCOL - 1) * jnp.log(3.0) + jax.random.uniform(subkeys[1], (ORDER,)) * jnp.log(3.3))
    noise = jnp.clip(jax.random.normal(subkeys[2], (ORDER, ORDER), jnp.float32), -6.0, 6.0)
    return (noise * row_scale[:, None] * col_scale[None, :]).astype(jnp.float32)


def level_of(key, dims, cuts, smallest, high):
    def one(dim, parts):
        heights = jax.random.uniform(jax.random.fold_in(jax.random.fold_in(key, 6), dim), (parts,), jnp.float32, smallest / len(cuts), high / len(cuts))
        return jnp.repeat(jnp.exp(heights), dims[dim] // parts).reshape((-1,) + (1,) * (len(dims) - dim - 1))

    level = one(*cuts[0])
    for cut in cuts[1:]:
        level = level * one(*cut)
    return level


def centred(stream_key, extent, spread, reach, cuts=(), dtype=jnp.bfloat16):
    loudness = level_of(stream_key, extent, cuts, -0.22, 0.18) if cuts else 1.0
    result = jax.random.normal(stream_key, extent, jnp.float32) * spread * loudness
    return jnp.minimum(jnp.maximum(result, -reach), reach).astype(dtype)


def setup_inputs(seed: int = 0) -> dict:
    key_of = jax.random.split(jax.random.key(seed), 4)
    return {
        "covariance": draw_covariance(jax.random.fold_in(key_of[3], 71), 0),
        "factor_left": centred(key_of[1], (RANK, ORDER), 1.0, 6.0, ((1, 32),), jnp.float32),
        "factor_right": centred(key_of[2], (RANK, ORDER), 0.5, 3.0, ((0, 4), (1, 8)), jnp.float32),
    }


epsilon = 1e-06

def reference(covariance, factor_left, factor_right):
    grid_rows = N_PROW
    grid_cols = N_PCOL
    tiles_down = ORDER // (TILE * grid_rows)
    tiles_across = ORDER // (TILE * grid_cols)
    natural = factor_right.reshape(RANK, grid_cols, tiles_across, TILE).transpose(0, 2, 1, 3).reshape(RANK, ORDER)
    corrected = covariance + jnp.dot(factor_left.T, natural, precision=lax.Precision.HIGHEST, preferred_element_type=jnp.float32)
    squared = corrected * corrected
    row_mean = lax.optimization_barrier(jnp.sum(squared, axis=1)) / ORDER + epsilon
    col_mean = lax.optimization_barrier(jnp.sum(squared, axis=0)) / ORDER + epsilon
    scaled = corrected * lax.rsqrt(jnp.sqrt(row_mean[:, None] * col_mean[None, :]))
    placed = scaled.reshape(tiles_down, grid_rows, TILE, tiles_across, grid_cols, TILE)
    return placed.transpose(1, 0, 2, 4, 3, 5).reshape(ORDER, ORDER)
```

```python
import functools

import jax
import jax.numpy as jnp
from jax import lax
from jax.experimental import pallas as pl
from jax.experimental.pallas import tpu as pltpu
from jax.sharding import PartitionSpec as P

ORDER = 16384
TILE = 64


epsilon = 1e-06


def deal_columns(source):
    height = source.shape[0]
    breadth = source.shape[1]
    grid_cols = lax.axis_size("pcol")
    arranged = (
        source.reshape(height, breadth // (TILE * grid_cols), grid_cols, TILE)
        .transpose(0, 2, 1, 3)
        .reshape(height, breadth)
    )
    return lax.all_to_all(arranged, "pcol", split_axis=1, concat_axis=0, tiled=True)


def order_rows(source):
    height = source.shape[0]
    breadth = source.shape[1]
    grid_rows = lax.axis_size("prow")
    grouped = source.reshape(height // (TILE * grid_rows), grid_rows, TILE, breadth)
    return grouped.transpose(1, 0, 2, 3).reshape(height, breadth)


def body(covariance, factor_left, factor_right):
    right_panel = lax.all_gather(factor_right, "prow", axis=0, tiled=True)
    dealt = deal_columns(covariance)
    left_block = lax.all_gather(factor_left, "pcol", axis=1, tiled=True).T
    tiles_moved, left_rows = (
        lax.all_to_all(order_rows(dealt), "prow", split_axis=0, concat_axis=0, tiled=True),
        lax.all_to_all(order_rows(left_block), "prow", split_axis=0, concat_axis=0, tiled=True),
    )
    corrected = tiles_moved + jnp.dot(
        left_rows, right_panel, precision=lax.Precision.HIGHEST, preferred_element_type=jnp.float32
    )
    squared = corrected * corrected
    row_total = lax.psum(jnp.sum(squared, axis=1), "pcol")
    col_total = lax.psum(jnp.sum(squared, axis=0), "prow")
    row_mean = row_total / ORDER + epsilon
    col_mean = col_total / ORDER + epsilon
    return corrected * lax.rsqrt(jnp.sqrt(row_mean[:, None] * col_mean[None, :]))


def flip(index, size, bits):
    out, unit = 0, 1
    while unit < size:
        out = out + unit * ((index // unit + bits // unit) % 2)
        unit *= 2
    return out


SLAB = TILE // 2
LANES = 128
CHUNK = 256
STAGES = 4


def deal_slab(grid_cols, src, dst):
    low = lax.broadcasted_iota(jnp.int32, (src.shape[0], LANES), 1) < TILE
    for pair in range(grid_cols // 2):
        for m in range(src.shape[1] // (LANES * grid_cols)):
            at = (pair + grid_cols * m) * LANES
            first = src[:, at:at + LANES]
            at += grid_cols // 2 * LANES
            second = src[:, at:at + LANES]
            dst[2 * pair, :, m * LANES:(m + 1) * LANES] = jnp.where(low, first, pltpu.roll(second, TILE, 1))
            dst[2 * pair + 1, :, m * LANES:(m + 1) * LANES] = jnp.where(low, pltpu.roll(first, TILE, 1), second)


def exchange_kernel(
    grid_rows, grid_cols,
    cov, left, right, got, row_parts, col_parts, tiles,
    slab_in, slab_out, left_own, lefts, rights, right_split, col_sum,
    in_sem, out_sem, tile_send, tile_recv, plane_send, plane_recv, block_send, block_recv,
    relay_send, relay_recv, swap_send, swap_recv, right_send, right_recv, own_sem,
    row_send, row_recv, col_send, col_recv,
):
    chips = grid_cols // 2
    p, q = lax.axis_index("prow"), lax.axis_index("pcol")
    z, core = q // 2, q % 2
    height = tiles.shape[2]
    rank = left.shape[0]
    beside = (z + z // 2) % 2
    half = z // 2
    mate = flip(z, chips, 1)
    far = jnp.maximum(z, 3 - z)

    def copy(src, dst, send, recv, to):
        return pltpu.make_async_remote_copy(
            src_ref=src, dst_ref=dst, send_sem=send, recv_sem=recv,
            device_id=to, device_id_type=pl.DeviceIdType.MESH,
        )

    def target(dp, dz, dc):
        return flip(p, grid_rows, dp), 2 * flip(z, chips, dz) + (core + dc) % 2

    barrier = pltpu.get_barrier_semaphore()
    for dp in range(grid_rows):
        for dz in range(chips):
            for dc in range(2):
                if (dp, dz, dc) != (0, 0, 0):
                    pl.semaphore_signal(
                        barrier, inc=1, device_id=target(dp, dz, dc), device_id_type=pl.DeviceIdType.MESH
                    )

    def slab_load(t, h):
        at = ((t % 2) * grid_rows + flip(p, grid_rows, t // 2)) * TILE + h * SLAB
        return pltpu.make_async_copy(cov.at[pl.ds(pl.multiple_of(at, SLAB), SLAB)], slab_in.at[h], in_sem.at[h])

    def slab_store(t, h):
        at = (t % 2) * TILE + h * SLAB
        return pltpu.make_async_copy(
            slab_out.at[t % 2, h],
            tiles.at[flip(p, grid_rows, t // 2), :, pl.ds(pl.multiple_of(at, SLAB), SLAB)],
            out_sem.at[t % 2, h],
        )

    for h in range(2):
        slab_load(0, h).start()

    low = lax.broadcasted_iota(jnp.int32, (rank, LANES), 1) < TILE
    for to in range(grid_rows):
        at = to // 2 * LANES
        first = left[:, at:at + LANES]
        at += grid_rows * TILE
        second = left[:, at:at + LANES]
        if to % 2 == 0:
            left_own[to] = jnp.where(low, first, pltpu.roll(second, TILE, 1))
        else:
            left_own[to] = jnp.where(low, pltpu.roll(first, TILE, 1), second)

    def plane(dp):
        return copy(
            left_own.at[flip(p, grid_rows, dp)], lefts.at[core, z, p],
            plane_send.at[dp], plane_recv.at[dp], target(dp, 0, 0),
        )

    def beside_right(dp):
        return copy(right, rights.at[p], right_send.at[dp], right_recv.at[dp], target(dp, 0, 0))

    keep_left = pltpu.make_async_copy(left_own.at[p], lefts.at[core, z, p], own_sem.at[0])
    keep_right = pltpu.make_async_copy(right, rights.at[p], own_sem.at[1])

    block = lefts.at[core, z]
    gate = 2 - half
    to_mate = copy(block, block, block_send.at[0], block_recv.at[z], (p, 2 * mate + core))
    to_gate = copy(block, block, block_send.at[1], block_recv.at[z], (p, 2 * gate + core))
    other = lefts.at[core, pl.ds(2 * (1 - half), 2)]
    relay = copy(other, other, relay_send, relay_recv, (p, 2 * mate + core))
    swap = copy(lefts.at[core], lefts.at[core], swap_send, swap_recv, target(0, 0, 1))
    own_rows = pl.ds(pl.multiple_of((p * grid_cols + q) * height, height), height)
    keep_tiles = pltpu.make_async_copy(tiles.at[p, q], got.at[own_rows], own_sem.at[2])

    def tile(dp, dz, dc, k):
        to = target(dp, dz, dc)
        at = (p * grid_cols + q) * height + k * TILE
        n = ((dp * chips + dz) * 2 + dc) * 2 + k
        return copy(
            tiles.at[to[0], to[1], pl.ds(pl.multiple_of(k * TILE, TILE), TILE)],
            got.at[pl.ds(pl.multiple_of(at, TILE), TILE)], tile_send.at[n], tile_recv.at[n], to,
        )

    def send_tiles(t, kind):
        dp, k = t // 2, t % 2
        for i in range(2):
            dz = kind * (3 - i) + (1 - kind) * (1 - i)
            for dc in range(2):
                mine = (dp + dz + dc) == 0

                @pl.when(jnp.logical_not(mine))
                def _():
                    tile(dp, dz, dc, k).start()

    def deal(t, carry):
        @pl.when(t < 2 * grid_rows)
        def _():
            for h in range(2):
                slab_load(t, h).wait()
                deal_slab(grid_cols, slab_in.at[h], slab_out.at[t % 2, h])

                @pl.when(t + 1 < 2 * grid_rows)
                def _():
                    slab_load(t + 1, h).start()

                slab_store(t, h).start()

                @pl.when((t == 0) & (h == 0))
                def _():
                    pl.semaphore_wait(barrier, grid_rows * grid_cols - 1)
                    keep_left.start()
                    for dp in range(1, grid_rows):
                        plane(dp).start()
                    keep_right.start()
                    for dp in range(1, grid_rows):
                        beside_right(dp).start()

        @pl.when(t == 0)
        def _():
            keep_left.wait()
            for dp in range(1, grid_rows):
                plane(dp).wait()
            to_gate.start()
            to_mate.start()

        @pl.when(t != 1)
        def _():
            s = jnp.maximum(t - 1, 0)
            for h in range(2):
                slab_store(s, h).wait()
            send_tiles(s, beside)

        return carry

    lax.fori_loop(0, 2 * grid_rows + 1, deal, 0)
    keep_tiles.start()

    to_gate.wait_send()
    to_mate.wait_send()

    def arrived(which):
        there = lefts.at[core, which]
        return copy(there, there, block_send.at[0], block_recv.at[which], (p, 2 * mate + core))

    arrived(mate).wait_recv()

    @pl.when(beside == 1)
    def _():
        for i in range(2):
            arrived(2 * (1 - half) + i).wait_recv()
        relay.start()

    def send_rest(t, carry):
        send_tiles(t, 1 - beside)
        return carry

    lax.fori_loop(0, 2 * grid_rows, send_rest, 0)

    keep_right.wait()
    for dp in range(1, grid_rows):
        beside_right(dp).wait()
    depth = right.shape[0]
    for n in range(grid_rows):
        value = rights[n]
        high = value.astype(jnp.bfloat16)
        rest = (value - high.astype(jnp.float32)).astype(jnp.bfloat16)
        right_split[n * depth:(n + 1) * depth] = high
        right_split[rank + n * depth:rank + (n + 1) * depth] = rest
        right_split[2 * rank + n * depth:2 * rank + (n + 1) * depth] = high
        right_split[3 * rank + n * depth:3 * rank + (n + 1) * depth] = jnp.zeros_like(high)
    col_sum[...] = jnp.zeros_like(col_sum)

    @pl.when(beside == 0)
    def _():
        relay.wait_recv()

    @pl.when(beside == 1)
    def _():
        relay.wait_send()

    swap.start()
    swap.wait()
    keep_tiles.wait()

    width = got.shape[1]

    def settle(m, carry):
        group = m // (2 * grid_rows)
        dz = jnp.where(group == 3, far, jnp.where(group == 2, 5 - far, group))
        dp, dc = m % (2 * grid_rows) // 2, m % 2
        from_p, from_q = target(dp, dz, dc)
        slot = from_p * grid_cols + from_q

        @pl.when(dp + dz + dc != 0)
        def _():
            for k in range(2):
                n = ((dp * chips + dz) * 2 + dc) * 2 + k
                there = got.at[pl.ds(pl.multiple_of(slot * height + k * TILE, TILE), TILE)]
                copy(
                    tiles.at[0, 0, pl.ds(0, TILE)], there, tile_send.at[n], tile_recv.at[n], (from_p, from_q)
                ).wait_recv()

        value = lefts[from_q % 2, from_q // 2, from_p]
        high = value.astype(jnp.bfloat16).astype(jnp.float32)
        stack = jnp.concatenate([high, high, value - high, jnp.zeros_like(high)], axis=0)
        factor = stack.T.astype(jnp.bfloat16)
        rows = pl.ds(pl.multiple_of(slot * height, height), height)
        total = jnp.zeros((height, LANES), jnp.float32)
        for at in range(0, width, CHUNK):
            here = slice(at, at + CHUNK)
            fixed = got[rows, here] + jnp.dot(
                factor, right_split[:, here], preferred_element_type=jnp.float32
            )
            got[rows, here] = fixed
            square = fixed * fixed
            for lane in range(0, CHUNK, LANES):
                total = total + square[:, lane:lane + LANES]
            part = square[0:8]
            for n in range(8, height, 8):
                part = part + square[n:n + 8]
            col_sum[:, here] += part
        row_parts[q, pl.ds(slot, 1)] = jnp.sum(total.T, axis=0, keepdims=True)
        return carry

    lax.fori_loop(0, grid_rows * grid_cols, settle, 0)
    col_parts[p] = jnp.sum(col_sum[...], axis=0, keepdims=True)

    def row_part(n):
        dz, dc = n // 2, n % 2
        return copy(row_parts.at[q], row_parts.at[q], row_send.at[n], row_recv.at[n], target(0, dz, dc))

    def col_part(dp):
        return copy(col_parts.at[p], col_parts.at[p], col_send.at[dp], col_recv.at[dp], target(dp, 0, 0))

    for n in range(grid_cols - 1, 0, -1):
        row_part(n).start()
    for dp in range(1, grid_rows):
        col_part(dp).start()

    def drain(n, carry):
        @pl.when(n > 1)
        def _():
            tile(n // (4 * chips), n // 4 % chips, n // 2 % 2, n % 2).wait_send()

        return carry

    lax.fori_loop(0, 2 * grid_rows * grid_cols, drain, 0)
    for n in range(1, grid_cols):
        row_part(n).wait()
    for dp in range(1, grid_rows):
        col_part(dp).wait()


def exchange(covariance, left, right):
    grid_rows, grid_cols = lax.axis_size("prow"), lax.axis_size("pcol")
    everyone = grid_rows * grid_cols
    rows, breadth = covariance.shape
    rank = left.shape[0]
    height, width = rows // grid_rows, breadth // grid_cols
    dma = pltpu.SemaphoreType.DMA
    vmem = pl.BlockSpec(memory_space=pltpu.VMEM)
    hbm = pl.BlockSpec(memory_space=pltpu.HBM)
    return pl.pallas_call(
        functools.partial(exchange_kernel, grid_rows, grid_cols),
        out_shape=(
            pltpu.VMEM((everyone * height, width), jnp.float32),
            pltpu.VMEM((grid_cols, everyone, height), jnp.float32),
            pltpu.VMEM((grid_rows, 1, width), jnp.float32),
            pltpu.HBM((grid_rows, grid_cols, height, width), jnp.float32),
        ),
        in_specs=[hbm, vmem, vmem],
        out_specs=(vmem, vmem, vmem, hbm),
        scratch_shapes=[
            pltpu.VMEM((2, SLAB, breadth), jnp.float32),
            pltpu.VMEM((2, 2, grid_cols, SLAB, width), jnp.float32),
            pltpu.VMEM((grid_rows, rank, height), jnp.float32),
            pltpu.VMEM((2, grid_cols // 2, grid_rows, rank, height), jnp.float32),
            pltpu.VMEM((grid_rows,) + right.shape, jnp.float32),
            pltpu.VMEM((4 * rank, width), jnp.bfloat16),
            pltpu.VMEM((8, width), jnp.float32),
            dma((2,)), dma((2, 2)), dma((2 * everyone,)), dma((2 * everyone,)),
            dma((grid_rows,)), dma((grid_rows,)), dma((2,)), dma((grid_cols // 2,)),
            dma, dma, dma, dma, dma((grid_rows,)), dma((grid_rows,)), dma((3,)),
            dma((grid_cols,)), dma((grid_cols,)), dma((grid_rows,)), dma((grid_rows,)),
        ],
        compiler_params=pltpu.CompilerParams(
            collective_id=0, has_side_effects=True, vmem_limit_bytes=22 * 1024 * 1024
        ),
    )(covariance, left, right)


def scale_kernel(order, got, row_parts, col_parts, out, stage, row_scale, sem):
    grid_cols, everyone, height = row_parts.shape
    width = got.shape[1]
    rows, cols = row_parts[0], col_parts[0]
    for n in range(1, grid_cols):
        rows = rows + row_parts[n]
    for n in range(1, col_parts.shape[0]):
        cols = cols + col_parts[n]
    row_scale[...] = lax.rsqrt(jnp.sqrt(rows / order + epsilon))
    col_scale = lax.rsqrt(jnp.sqrt(cols / order + epsilon))

    def store(n):
        return pltpu.make_async_copy(
            stage.at[n % STAGES], out.at[pl.ds(pl.multiple_of(n * height, height), height)], sem.at[n % STAGES]
        )

    def step(n, carry):
        @pl.when(n >= STAGES)
        def _():
            store(n - STAGES).wait()

        scale = jnp.broadcast_to(row_scale[pl.ds(n, 1)], (height, height)).T
        here = pl.ds(pl.multiple_of(n * height, height), height)
        for at in range(0, width, LANES):
            stage[n % STAGES, :, at:at + LANES] = got[here, at:at + LANES] * scale * col_scale[:, at:at + LANES]
        store(n).start()
        return carry

    lax.fori_loop(0, everyone, step, 0)
    for n in range(everyone - STAGES, everyone):
        store(n).wait()


def scaled(order, got, row_parts, col_parts):
    height, width = row_parts.shape[2], got.shape[1]
    vmem = pl.BlockSpec(memory_space=pltpu.VMEM)
    return pl.pallas_call(
        functools.partial(scale_kernel, order),
        out_shape=jax.ShapeDtypeStruct(got.shape, jnp.float32),
        in_specs=[vmem] * 3,
        out_specs=pl.BlockSpec(memory_space=pl.ANY),
        scratch_shapes=[
            pltpu.VMEM((STAGES, height, width), jnp.float32),
            pltpu.VMEM(row_parts.shape[1:], jnp.float32),
            pltpu.SemaphoreType.DMA((STAGES,)),
        ],
        compiler_params=pltpu.CompilerParams(vmem_limit_bytes=12 * 1024 * 1024),
    )(got, row_parts, col_parts)


def direct_body(covariance, factor_left, factor_right):
    got, row_parts, col_parts, _ = exchange(covariance, factor_left, factor_right)
    held = [pltpu.with_memory_space_constraint(x, pltpu.VMEM) for x in (got, row_parts, col_parts)]
    return scaled(covariance.shape[1], *held)


def power_of_two(n):
    return n & (n - 1) == 0


def chosen(mesh, covariance):
    grid_rows, grid_cols = mesh.shape["prow"], mesh.shape["pcol"]
    tiles = covariance.shape[0] // (grid_rows * grid_cols * TILE)
    fits = tiles == 2 * grid_rows and grid_cols == 8
    across = covariance.shape[1] // (TILE * grid_cols)
    fits = fits and power_of_two(grid_rows) and grid_rows > 1 and across % 4 == 0
    return direct_body if fits else body


def solution(mesh):
    placed = (P(("prow", "pcol"), None), P(None, ("prow", "pcol")), P("prow", "pcol"))

    def run(covariance, factor_left, factor_right):
        return jax.shard_map(
            chosen(mesh, covariance), mesh=mesh, in_specs=placed, out_specs=P("prow", "pcol"), check_vma=False
        )(covariance, factor_left, factor_right)

    return run
```

```python
import functools

import jax
import jax.numpy as jnp
from jax import lax
from jax.experimental import pallas as pl
from jax.experimental.pallas import tpu as pltpu
from jax.sharding import PartitionSpec as P

ORDER = 16384
TILE = 64


epsilon = 1e-06


def deal_columns(source):
    height = source.shape[0]
    breadth = source.shape[1]
    grid_cols = lax.axis_size("pcol")
    arranged = (
        source.reshape(height, breadth // (TILE * grid_cols), grid_cols, TILE)
        .transpose(0, 2, 1, 3)
        .reshape(height, breadth)
    )
    return lax.all_to_all(arranged, "pcol", split_axis=1, concat_axis=0, tiled=True)


def order_rows(source):
    height = source.shape[0]
    breadth = source.shape[1]
    grid_rows = lax.axis_size("prow")
    grouped = source.reshape(height // (TILE * grid_rows), grid_rows, TILE, breadth)
    return grouped.transpose(1, 0, 2, 3).reshape(height, breadth)


def body(covariance, factor_left, factor_right):
    right_panel = lax.all_gather(factor_right, "prow", axis=0, tiled=True)
    dealt = deal_columns(covariance)
    left_block = lax.all_gather(factor_left, "pcol", axis=1, tiled=True).T
    tiles_moved, left_rows = (
        lax.all_to_all(order_rows(dealt), "prow", split_axis=0, concat_axis=0, tiled=True),
        lax.all_to_all(order_rows(left_block), "prow", split_axis=0, concat_axis=0, tiled=True),
    )
    corrected = tiles_moved + jnp.dot(
        left_rows, right_panel, precision=lax.Precision.HIGHEST, preferred_element_type=jnp.float32
    )
    squared = corrected * corrected
    row_total = lax.psum(jnp.sum(squared, axis=1), "pcol")
    col_total = lax.psum(jnp.sum(squared, axis=0), "prow")
    row_mean = row_total / ORDER + epsilon
    col_mean = col_total / ORDER + epsilon
    return corrected * lax.rsqrt(jnp.sqrt(row_mean[:, None] * col_mean[None, :]))


def flip(index, size, bits):
    out, unit = 0, 1
    while unit < size:
        out = out + unit * ((index // unit + bits // unit) % 2)
        unit *= 2
    return out


SLAB = TILE // 2
LANES = 128
CHUNK = 256
STAGES = 4
HELD = 26


def deal_slab(grid_cols, src, dst):
    low = lax.broadcasted_iota(jnp.int32, (src.shape[0], LANES), 1) < TILE
    for pair in range(grid_cols // 2):
        for m in range(src.shape[1] // (LANES * grid_cols)):
            at = (pair + grid_cols * m) * LANES
            first = src[:, at:at + LANES]
            at += grid_cols // 2 * LANES
            second = src[:, at:at + LANES]
            dst[2 * pair, :, m * LANES:(m + 1) * LANES] = jnp.where(low, first, pltpu.roll(second, TILE, 1))
            dst[2 * pair + 1, :, m * LANES:(m + 1) * LANES] = jnp.where(low, pltpu.roll(first, TILE, 1), second)


def exchange_kernel(
    grid_rows, grid_cols,
    cov, left, right, got, row_parts, col_parts, tiles,
    slab_in, slab_out, left_own, lefts, rights, right_split, col_sum,
    in_sem, out_sem, tile_send, tile_recv, plane_send, plane_recv, block_send, block_recv,
    relay_send, relay_recv, swap_send, swap_recv, right_send, right_recv, own_sem,
    row_send, row_recv, col_send, col_recv,
):
    chips = grid_cols // 2
    p, q = lax.axis_index("prow"), lax.axis_index("pcol")
    z, core = q // 2, q % 2
    height = tiles.shape[2]
    rank = left.shape[0]
    beside = (z + z // 2) % 2
    half = z // 2
    mate = flip(z, chips, 1)
    far = jnp.maximum(z, 3 - z)

    def copy(src, dst, send, recv, to):
        return pltpu.make_async_remote_copy(
            src_ref=src, dst_ref=dst, send_sem=send, recv_sem=recv,
            device_id=to, device_id_type=pl.DeviceIdType.MESH,
        )

    def target(dp, dz, dc):
        return flip(p, grid_rows, dp), 2 * flip(z, chips, dz) + (core + dc) % 2

    barrier = pltpu.get_barrier_semaphore()
    for dp in range(grid_rows):
        for dz in range(chips):
            for dc in range(2):
                if (dp, dz, dc) != (0, 0, 0):
                    pl.semaphore_signal(
                        barrier, inc=1, device_id=target(dp, dz, dc), device_id_type=pl.DeviceIdType.MESH
                    )

    def slab_load(t, h):
        at = ((t % 2) * grid_rows + flip(p, grid_rows, t // 2)) * TILE + h * SLAB
        return pltpu.make_async_copy(cov.at[pl.ds(pl.multiple_of(at, SLAB), SLAB)], slab_in.at[h], in_sem.at[h])

    def slab_slot(t):
        return jnp.where(t == 0, 2, t % 2)

    def slab_store(t, h):
        at = (t % 2) * TILE + h * SLAB
        return pltpu.make_async_copy(
            slab_out.at[slab_slot(t), h],
            tiles.at[flip(p, grid_rows, t // 2), :, pl.ds(pl.multiple_of(at, SLAB), SLAB)],
            out_sem.at[slab_slot(t), h],
        )

    for h in range(2):
        slab_load(0, h).start()

    low = lax.broadcasted_iota(jnp.int32, (rank, LANES), 1) < TILE
    for to in range(grid_rows):
        at = to // 2 * LANES
        first = left[:, at:at + LANES]
        at += grid_rows * TILE
        second = left[:, at:at + LANES]
        if to % 2 == 0:
            left_own[to] = jnp.where(low, first, pltpu.roll(second, TILE, 1))
        else:
            left_own[to] = jnp.where(low, pltpu.roll(first, TILE, 1), second)

    def plane(dp):
        return copy(
            left_own.at[flip(p, grid_rows, dp)], lefts.at[core, z, p],
            plane_send.at[dp], plane_recv.at[dp], target(dp, 0, 0),
        )

    def beside_right(dp):
        return copy(right, rights.at[p], right_send.at[dp], right_recv.at[dp], target(dp, 0, 0))

    keep_left = pltpu.make_async_copy(left_own.at[p], lefts.at[core, z, p], own_sem.at[0])
    keep_right = pltpu.make_async_copy(right, rights.at[p], own_sem.at[1])

    block = lefts.at[core, z]
    gate = 2 - half
    to_mate = copy(block, block, block_send.at[0], block_recv.at[z], (p, 2 * mate + core))
    to_gate = copy(block, block, block_send.at[1], block_recv.at[z], (p, 2 * gate + core))
    other = lefts.at[core, pl.ds(2 * (1 - half), 2)]
    relay = copy(other, other, relay_send, relay_recv, (p, 2 * mate + core))
    swap = copy(lefts.at[core], lefts.at[core], swap_send, swap_recv, target(0, 0, 1))
    own_rows = pl.ds(pl.multiple_of((p * grid_cols + q) * height, height), height)
    keep_tiles = pltpu.make_async_copy(tiles.at[p, q], got.at[own_rows], own_sem.at[2])

    def tile(dp, dz, dc, k):
        to = target(dp, dz, dc)
        at = (p * grid_cols + q) * height + k * TILE
        n = ((dp * chips + dz) * 2 + dc) * 2 + k
        return copy(
            tiles.at[to[0], to[1], pl.ds(pl.multiple_of(k * TILE, TILE), TILE)],
            got.at[pl.ds(pl.multiple_of(at, TILE), TILE)], tile_send.at[n], tile_recv.at[n], to,
        )

    def send_slab(h):
        at = pl.multiple_of((p * grid_cols + q) * height + h * SLAB, SLAB)
        for i in range(2):
            dz = beside * (3 - i) + (1 - beside) * (1 - i)
            for dc in range(2):
                to = target(0, dz, dc)
                n = (dz * 2 + dc) * 2

                @pl.when(dz + dc != 0)
                def _():
                    copy(
                        slab_out.at[2, h, to[1]], got.at[pl.ds(at, SLAB)], tile_send.at[n], tile_recv.at[n], to
                    ).start()

    def send_tiles(dp, kind, halves):
        for i in range(2):
            dz = kind * (3 - i) + (1 - kind) * (1 - i)
            for dc in range(2):

                @pl.when(dp + dz + dc != 0)
                def _():
                    for k in halves:
                        tile(dp, dz, dc, k).start()

    def deal(t, carry):
        @pl.when(t < 2 * grid_rows)
        def _():
            for h in range(2):
                slab_load(t, h).wait()
                deal_slab(grid_cols, slab_in.at[h], slab_out.at[slab_slot(t), h])

                @pl.when(t + 1 < 2 * grid_rows)
                def _():
                    slab_load(t + 1, h).start()

                slab_store(t, h).start()

                @pl.when((t == 0) & (h == 0))
                def _():
                    pl.semaphore_wait(barrier, grid_rows * grid_cols - 1)
                    send_slab(0)
                    keep_left.start()
                    for dp in range(1, grid_rows):
                        plane(dp).start()
                    keep_right.start()
                    for dp in range(1, grid_rows):
                        beside_right(dp).start()

                @pl.when((t == 0) & (h == 1))
                def _():
                    send_slab(1)

        @pl.when(t > 0)
        def _():
            for h in range(2):
                slab_store(t - 1, h).wait()

        @pl.when(t == 2)
        def _():
            send_tiles(0, beside, (1,))

        @pl.when(t == 0)
        def _():
            keep_left.wait()
            for dp in range(1, grid_rows):
                plane(dp).wait()
            to_gate.start()
            to_mate.start()

        @pl.when((t > 2) & (t % 2 == 0))
        def _():
            send_tiles(t // 2 - 1, beside, (0, 1))
            send_tiles(t // 2 - 2, 1 - beside, (0, 1))

        return carry

    lax.fori_loop(0, 2 * grid_rows + 1, deal, 0)
    keep_tiles.start()

    to_gate.wait_send()
    to_mate.wait_send()

    def arrived(which):
        there = lefts.at[core, which]
        return copy(there, there, block_send.at[0], block_recv.at[which], (p, 2 * mate + core))

    arrived(mate).wait_recv()

    @pl.when(beside == 1)
    def _():
        for i in range(2):
            arrived(2 * (1 - half) + i).wait_recv()
        relay.start()

    send_tiles(grid_rows - 1, 1 - beside, (0, 1))
    keep_right.wait()
    for dp in range(1, grid_rows):
        beside_right(dp).wait()
    depth = right.shape[0]
    for n in range(grid_rows):
        value = rights[n]
        high = value.astype(jnp.bfloat16)
        rest = (value - high.astype(jnp.float32)).astype(jnp.bfloat16)
        right_split[n * depth:(n + 1) * depth] = high
        right_split[rank + n * depth:rank + (n + 1) * depth] = rest
        right_split[2 * rank + n * depth:2 * rank + (n + 1) * depth] = high
        right_split[3 * rank + n * depth:3 * rank + (n + 1) * depth] = jnp.zeros_like(high)
    col_sum[...] = jnp.zeros_like(col_sum)

    @pl.when(beside == 0)
    def _():
        relay.wait_recv()

    @pl.when(beside == 1)
    def _():
        relay.wait_send()

    swap.start()
    swap.wait()
    keep_tiles.wait()

    width = got.shape[1]

    def settle(m, carry):
        group = m // (2 * grid_rows)
        dz = jnp.where(group == 3, 5 - far, jnp.where(group == 2, far, group))
        dp, dc = m % (2 * grid_rows) // 2, m % 2
        from_p, from_q = target(dp, dz, dc)
        slot = from_p * grid_cols + from_q

        @pl.when(dp + dz + dc != 0)
        def _():
            for k in range(2):
                n = ((dp * chips + dz) * 2 + dc) * 2 + k
                there = got.at[pl.ds(pl.multiple_of(slot * height + k * TILE, TILE), TILE)]
                copy(
                    tiles.at[0, 0, pl.ds(0, TILE)], there, tile_send.at[n], tile_recv.at[n], (from_p, from_q)
                ).wait_recv()

        value = lefts[from_q % 2, from_q // 2, from_p]
        high = value.astype(jnp.bfloat16).astype(jnp.float32)
        stack = jnp.concatenate([high, high, value - high, jnp.zeros_like(high)], axis=0)
        factor = stack.T.astype(jnp.bfloat16)
        rows = pl.ds(pl.multiple_of(slot * height, height), height)
        total = jnp.zeros((height, LANES), jnp.float32)
        for at in range(0, width, CHUNK):
            here = slice(at, at + CHUNK)
            fixed = got[rows, here] + jnp.dot(
                factor, right_split[:, here], preferred_element_type=jnp.float32
            )
            got[rows, here] = fixed
            square = fixed * fixed
            for lane in range(0, CHUNK, LANES):
                total = total + square[:, lane:lane + LANES]
            part = square[0:8]
            for n in range(8, height, 8):
                part = part + square[n:n + 8]
            col_sum[:, here] += part
        row_parts[q, pl.ds(slot, 1)] = jnp.sum(total.T, axis=0, keepdims=True)
        return carry

    lax.fori_loop(0, grid_rows * grid_cols, settle, 0)
    col_parts[p] = jnp.sum(col_sum[...], axis=0, keepdims=True)

    def row_part(n):
        dz, dc = n // 2, n % 2
        return copy(row_parts.at[q], row_parts.at[q], row_send.at[n], row_recv.at[n], target(0, dz, dc))

    def col_part(dp):
        return copy(col_parts.at[p], col_parts.at[p], col_send.at[dp], col_recv.at[dp], target(dp, 0, 0))

    for n in range(grid_cols - 1, 0, -1):
        row_part(n).start()
    for dp in range(1, grid_rows):
        col_part(dp).start()

    def drain(n, carry):
        @pl.when(n > 1)
        def _():
            tile(n // (4 * chips), n // 4 % chips, n // 2 % 2, n % 2).wait_send()

        return carry

    lax.fori_loop(0, 2 * grid_rows * grid_cols, drain, 0)
    for n in range(1, grid_cols):
        row_part(n).wait()
    for dp in range(1, grid_rows):
        col_part(dp).wait()


def exchange(covariance, left, right):
    grid_rows, grid_cols = lax.axis_size("prow"), lax.axis_size("pcol")
    everyone = grid_rows * grid_cols
    rows, breadth = covariance.shape
    rank = left.shape[0]
    height, width = rows // grid_rows, breadth // grid_cols
    dma = pltpu.SemaphoreType.DMA
    vmem = pl.BlockSpec(memory_space=pltpu.VMEM)
    hbm = pl.BlockSpec(memory_space=pltpu.HBM)
    return pl.pallas_call(
        functools.partial(exchange_kernel, grid_rows, grid_cols),
        out_shape=(
            pltpu.VMEM((everyone * height, width), jnp.float32),
            pltpu.VMEM((grid_cols, everyone, height), jnp.float32),
            pltpu.VMEM((grid_rows, 1, width), jnp.float32),
            pltpu.HBM((grid_rows, grid_cols, height, width), jnp.float32),
        ),
        in_specs=[hbm, vmem, vmem],
        out_specs=(vmem, vmem, vmem, hbm),
        scratch_shapes=[
            pltpu.VMEM((2, SLAB, breadth), jnp.float32),
            pltpu.VMEM((3, 2, grid_cols, SLAB, width), jnp.float32),
            pltpu.VMEM((grid_rows, rank, height), jnp.float32),
            pltpu.VMEM((2, grid_cols // 2, grid_rows, rank, height), jnp.float32),
            pltpu.VMEM((grid_rows,) + right.shape, jnp.float32),
            pltpu.VMEM((4 * rank, width), jnp.bfloat16),
            pltpu.VMEM((8, width), jnp.float32),
            dma((2,)), dma((3, 2)), dma((2 * everyone,)), dma((2 * everyone,)),
            dma((grid_rows,)), dma((grid_rows,)), dma((2,)), dma((grid_cols // 2,)),
            dma, dma, dma, dma, dma((grid_rows,)), dma((grid_rows,)), dma((3,)),
            dma((grid_cols,)), dma((grid_cols,)), dma((grid_rows,)), dma((grid_rows,)),
        ],
        compiler_params=pltpu.CompilerParams(
            collective_id=0, has_side_effects=True, vmem_limit_bytes=HELD * 1024 * 1024
        ),
    )(covariance, left, right)


def scale_kernel(order, got, row_parts, col_parts, out, stage, row_scale, sem):
    grid_cols, everyone, height = row_parts.shape
    width = got.shape[1]
    rows, cols = row_parts[0], col_parts[0]
    for n in range(1, grid_cols):
        rows = rows + row_parts[n]
    for n in range(1, col_parts.shape[0]):
        cols = cols + col_parts[n]
    row_scale[...] = lax.rsqrt(jnp.sqrt(rows / order + epsilon))
    col_scale = lax.rsqrt(jnp.sqrt(cols / order + epsilon))

    def store(n):
        return pltpu.make_async_copy(
            stage.at[n % STAGES], out.at[pl.ds(pl.multiple_of(n * height, height), height)], sem.at[n % STAGES]
        )

    def step(n, carry):
        @pl.when(n >= STAGES)
        def _():
            store(n - STAGES).wait()

        scale = jnp.broadcast_to(row_scale[pl.ds(n, 1)], (height, height)).T
        here = pl.ds(pl.multiple_of(n * height, height), height)
        for at in range(0, width, LANES):
            stage[n % STAGES, :, at:at + LANES] = got[here, at:at + LANES] * scale * col_scale[:, at:at + LANES]
        store(n).start()
        return carry

    lax.fori_loop(0, everyone, step, 0)
    for n in range(everyone - STAGES, everyone):
        store(n).wait()


def scaled(order, got, row_parts, col_parts):
    height, width = row_parts.shape[2], got.shape[1]
    vmem = pl.BlockSpec(memory_space=pltpu.VMEM)
    return pl.pallas_call(
        functools.partial(scale_kernel, order),
        out_shape=jax.ShapeDtypeStruct(got.shape, jnp.float32),
        in_specs=[vmem] * 3,
        out_specs=pl.BlockSpec(memory_space=pl.ANY),
        scratch_shapes=[
            pltpu.VMEM((STAGES, height, width), jnp.float32),
            pltpu.VMEM(row_parts.shape[1:], jnp.float32),
            pltpu.SemaphoreType.DMA((STAGES,)),
        ],
        compiler_params=pltpu.CompilerParams(vmem_limit_bytes=HELD * 1024 * 1024),
    )(got, row_parts, col_parts)


def direct_body(covariance, factor_left, factor_right):
    got, row_parts, col_parts, _ = exchange(covariance, factor_left, factor_right)
    held = [pltpu.with_memory_space_constraint(x, pltpu.VMEM) for x in (got, row_parts, col_parts)]
    return scaled(covariance.shape[1], *held)


def power_of_two(n):
    return n & (n - 1) == 0


def chosen(mesh, covariance):
    grid_rows, grid_cols = mesh.shape["prow"], mesh.shape["pcol"]
    tiles = covariance.shape[0] // (grid_rows * grid_cols * TILE)
    fits = tiles == 2 * grid_rows and grid_cols == 8
    across = covariance.shape[1] // (TILE * grid_cols)
    fits = fits and power_of_two(grid_rows) and grid_rows > 1 and across % 4 == 0
    return direct_body if fits else body


def solution(mesh):
    placed = (P(("prow", "pcol"), None), P(None, ("prow", "pcol")), P("prow", "pcol"))

    def run(covariance, factor_left, factor_right):
        return jax.shard_map(
            chosen(mesh, covariance), mesh=mesh, in_specs=placed, out_specs=P("prow", "pcol"), check_vma=False
        )(covariance, factor_left, factor_right)

    return run
```

```python
import functools

import jax
import jax.numpy as jnp
from jax import lax
from jax.experimental import pallas as pl
from jax.experimental.pallas import tpu as pltpu
from jax.sharding import PartitionSpec as P

ORDER = 16384
TILE = 64


epsilon = 1e-06


def deal_columns(source):
    height = source.shape[0]
    breadth = source.shape[1]
    grid_cols = lax.axis_size("pcol")
    arranged = (
        source.reshape(height, breadth // (TILE * grid_cols), grid_cols, TILE)
        .transpose(0, 2, 1, 3)
        .reshape(height, breadth)
    )
    return lax.all_to_all(arranged, "pcol", split_axis=1, concat_axis=0, tiled=True)


def order_rows(source):
    height = source.shape[0]
    breadth = source.shape[1]
    grid_rows = lax.axis_size("prow")
    grouped = source.reshape(height // (TILE * grid_rows), grid_rows, TILE, breadth)
    return grouped.transpose(1, 0, 2, 3).reshape(height, breadth)


def body(covariance, factor_left, factor_right):
    right_panel = lax.all_gather(factor_right, "prow", axis=0, tiled=True)
    dealt = deal_columns(covariance)
    left_block = lax.all_gather(factor_left, "pcol", axis=1, tiled=True).T
    tiles_moved, left_rows = (
        lax.all_to_all(order_rows(dealt), "prow", split_axis=0, concat_axis=0, tiled=True),
        lax.all_to_all(order_rows(left_block), "prow", split_axis=0, concat_axis=0, tiled=True),
    )
    corrected = tiles_moved + jnp.dot(
        left_rows, right_panel, precision=lax.Precision.HIGHEST, preferred_element_type=jnp.float32
    )
    squared = corrected * corrected
    row_total = lax.psum(jnp.sum(squared, axis=1), "pcol")
    col_total = lax.psum(jnp.sum(squared, axis=0), "prow")
    row_mean = row_total / ORDER + epsilon
    col_mean = col_total / ORDER + epsilon
    return corrected * lax.rsqrt(jnp.sqrt(row_mean[:, None] * col_mean[None, :]))


def flip(index, size, bits):
    out, unit = 0, 1
    while unit < size:
        out = out + unit * ((index // unit + bits // unit) % 2)
        unit *= 2
    return out


SLAB = TILE // 2
LANES = 128
CHUNK = 256
STAGES = 4
HELD = 26


def deal_slab(grid_cols, src, dst):
    low = lax.broadcasted_iota(jnp.int32, (src.shape[0], LANES), 1) < TILE
    for pair in range(grid_cols // 2):
        for m in range(src.shape[1] // (LANES * grid_cols)):
            at = (pair + grid_cols * m) * LANES
            first = src[:, at:at + LANES]
            at += grid_cols // 2 * LANES
            second = src[:, at:at + LANES]
            dst[2 * pair, :, m * LANES:(m + 1) * LANES] = jnp.where(low, first, pltpu.roll(second, TILE, 1))
            dst[2 * pair + 1, :, m * LANES:(m + 1) * LANES] = jnp.where(low, pltpu.roll(first, TILE, 1), second)


def exchange_kernel(
    grid_rows, grid_cols,
    cov, left, right, got, row_parts, col_parts, tiles,
    slab_in, slab_out, left_in, left_own, lefts, rights, right_split, col_sum,
    in_sem, out_sem, tile_send, tile_recv, plane_send, plane_recv, block_send, block_recv,
    relay_send, relay_recv, swap_send, swap_recv, right_send, right_recv, own_sem,
    row_send, row_recv, col_send, col_recv,
):
    chips = grid_cols // 2
    p, q = lax.axis_index("prow"), lax.axis_index("pcol")
    z, core = q // 2, q % 2
    height = tiles.shape[2]
    rank = left.shape[0]
    beside = (z + z // 2) % 2
    half = z // 2
    mate = flip(z, chips, 1)
    far = jnp.maximum(z, 3 - z)

    def copy(src, dst, send, recv, to):
        return pltpu.make_async_remote_copy(
            src_ref=src, dst_ref=dst, send_sem=send, recv_sem=recv,
            device_id=to, device_id_type=pl.DeviceIdType.MESH,
        )

    def target(dp, dz, dc):
        return flip(p, grid_rows, dp), 2 * flip(z, chips, dz) + (core + dc) % 2

    def slab_load(t, h):
        at = ((t % 2) * grid_rows + flip(p, grid_rows, t // 2)) * TILE + h * SLAB
        return pltpu.make_async_copy(cov.at[pl.ds(pl.multiple_of(at, SLAB), SLAB)], slab_in.at[h], in_sem.at[h])

    def slab_slot(t):
        return jnp.where(t == 0, 2, t % 2)

    def slab_store(t, h):
        at = (t % 2) * TILE + h * SLAB
        return pltpu.make_async_copy(
            slab_out.at[slab_slot(t), h],
            tiles.at[flip(p, grid_rows, t // 2), :, pl.ds(pl.multiple_of(at, SLAB), SLAB)],
            out_sem.at[slab_slot(t), h],
        )

    for h in range(2):
        slab_load(0, h).start()
    load_left = pltpu.make_async_copy(left, left_in, own_sem.at[3])
    load_left.start()

    barrier = pltpu.get_barrier_semaphore()
    for dp in range(grid_rows):
        for dz in range(chips):
            for dc in range(2):
                if (dp, dz, dc) != (0, 0, 0):
                    pl.semaphore_signal(
                        barrier, inc=1, device_id=target(dp, dz, dc), device_id_type=pl.DeviceIdType.MESH
                    )

    def pick_left():
        low = lax.broadcasted_iota(jnp.int32, (rank, LANES), 1) < TILE
        for to in range(grid_rows):
            at = to // 2 * LANES
            first = left_in[:, at:at + LANES]
            at += grid_rows * TILE
            second = left_in[:, at:at + LANES]
            if to % 2 == 0:
                left_own[to] = jnp.where(low, first, pltpu.roll(second, TILE, 1))
            else:
                left_own[to] = jnp.where(low, pltpu.roll(first, TILE, 1), second)

    def plane(dp):
        return copy(
            left_own.at[flip(p, grid_rows, dp)], lefts.at[core, z, p],
            plane_send.at[dp], plane_recv.at[dp], target(dp, 0, 0),
        )

    def beside_right(dp):
        return copy(right, rights.at[p], right_send.at[dp], right_recv.at[dp], target(dp, 0, 0))

    keep_left = pltpu.make_async_copy(left_own.at[p], lefts.at[core, z, p], own_sem.at[0])
    keep_right = pltpu.make_async_copy(right, rights.at[p], own_sem.at[1])

    block = lefts.at[core, z]
    gate = 2 - half
    to_mate = copy(block, block, block_send.at[0], block_recv.at[z], (p, 2 * mate + core))
    to_gate = copy(block, block, block_send.at[1], block_recv.at[z], (p, 2 * gate + core))
    other = lefts.at[core, pl.ds(2 * (1 - half), 2)]
    relay = copy(other, other, relay_send, relay_recv, (p, 2 * mate + core))
    swap = copy(lefts.at[core], lefts.at[core], swap_send, swap_recv, target(0, 0, 1))
    own_rows = pl.ds(pl.multiple_of((p * grid_cols + q) * height, height), height)
    keep_tiles = pltpu.make_async_copy(tiles.at[p, q], got.at[own_rows], own_sem.at[2])

    def tile(dp, dz, dc, start, count):
        to = target(dp, dz, dc)
        at = pl.multiple_of((p * grid_cols + q) * height + start, TILE)
        n = (dp * chips + dz) * 2 + dc
        return copy(
            tiles.at[to[0], to[1], pl.ds(start, count)], got.at[pl.ds(at, count)], tile_send.at[n], tile_recv.at[n], to
        )

    def send_slab(h):
        at = pl.multiple_of((p * grid_cols + q) * height + h * SLAB, SLAB)
        for i in range(2):
            dz = beside * (3 - i) + (1 - beside) * (1 - i)
            for dc in range(2):
                to = target(0, dz, dc)
                n = dz * 2 + dc

                @pl.when(dz + dc != 0)
                def _():
                    copy(
                        slab_out.at[2, h, to[1]], got.at[pl.ds(at, SLAB)], tile_send.at[n], tile_recv.at[n], to
                    ).start()

    def send_tiles(dp, kind, start=0):
        for i in range(2):
            dz = kind * (3 - i) + (1 - kind) * (1 - i)
            for dc in range(2):

                @pl.when(dp + dz + dc != 0)
                def _():
                    tile(dp, dz, dc, start, height - start).start()

    def deal(t, carry):
        @pl.when(t < 2 * grid_rows)
        def _():
            for h in range(2):
                slab_load(t, h).wait()
                deal_slab(grid_cols, slab_in.at[h], slab_out.at[slab_slot(t), h])

                @pl.when(t + 1 < 2 * grid_rows)
                def _():
                    slab_load(t + 1, h).start()

                slab_store(t, h).start()

                @pl.when((t == 0) & (h == 0))
                def _():
                    pl.semaphore_wait(barrier, grid_rows * grid_cols - 1)
                    send_slab(0)
                    load_left.wait()
                    pick_left()
                    keep_right.start()
                    for dp in range(1, grid_rows):
                        beside_right(dp).start()

                @pl.when((t == 0) & (h == 1))
                def _():
                    send_slab(1)
                    keep_left.start()
                    for dp in range(1, grid_rows):
                        plane(dp).start()

        @pl.when(t > 0)
        def _():
            for h in range(2):
                slab_store(t - 1, h).wait()

        @pl.when(t == 2)
        def _():
            send_tiles(0, beside, TILE)

        @pl.when(t == 1)
        def _():
            keep_left.wait()
            for dp in range(1, grid_rows):
                plane(dp).wait()
            to_gate.start()
            to_mate.start()

        @pl.when((t > 2) & (t % 2 == 0))
        def _():
            send_tiles(t // 2 - 1, beside)
            send_tiles(t // 2 - 2, 1 - beside)

        return carry

    lax.fori_loop(0, 2 * grid_rows + 1, deal, 0)
    keep_tiles.start()

    to_gate.wait_send()
    to_mate.wait_send()

    def arrived(which):
        there = lefts.at[core, which]
        return copy(there, there, block_send.at[0], block_recv.at[which], (p, 2 * mate + core))

    arrived(mate).wait_recv()

    @pl.when(beside == 1)
    def _():
        for i in range(2):
            arrived(2 * (1 - half) + i).wait_recv()
        relay.start()

    send_tiles(grid_rows - 1, 1 - beside)
    keep_right.wait()
    for dp in range(1, grid_rows):
        beside_right(dp).wait()
    depth = right.shape[0]
    for n in range(grid_rows):
        value = rights[n]
        high = value.astype(jnp.bfloat16)
        rest = (value - high.astype(jnp.float32)).astype(jnp.bfloat16)
        right_split[n * depth:(n + 1) * depth] = high
        right_split[rank + n * depth:rank + (n + 1) * depth] = rest
        right_split[2 * rank + n * depth:2 * rank + (n + 1) * depth] = high
        right_split[3 * rank + n * depth:3 * rank + (n + 1) * depth] = jnp.zeros_like(high)
    col_sum[...] = jnp.zeros_like(col_sum)

    @pl.when(beside == 0)
    def _():
        relay.wait_recv()

    @pl.when(beside == 1)
    def _():
        relay.wait_send()

    swap.start()
    swap.wait()
    keep_tiles.wait()

    width = got.shape[1]

    def settle(m, carry):
        group = m // (2 * grid_rows)
        dz = jnp.where(group == 3, 5 - far, jnp.where(group == 2, far, group))
        dp, dc = m % (2 * grid_rows) // 2, m % 2
        from_p, from_q = target(dp, dz, dc)
        slot = from_p * grid_cols + from_q

        @pl.when(dp + dz + dc != 0)
        def _():
            n = (dp * chips + dz) * 2 + dc
            there = got.at[pl.ds(pl.multiple_of(slot * height, height), height)]
            copy(tiles.at[0, 0], there, tile_send.at[n], tile_recv.at[n], (from_p, from_q)).wait_recv()

        value = lefts[from_q % 2, from_q // 2, from_p]
        high = value.astype(jnp.bfloat16).astype(jnp.float32)
        stack = jnp.concatenate([high, high, value - high, jnp.zeros_like(high)], axis=0)
        factor = stack.T.astype(jnp.bfloat16)
        rows = pl.ds(pl.multiple_of(slot * height, height), height)
        total = jnp.zeros((height, LANES), jnp.float32)
        for at in range(0, width, CHUNK):
            here = slice(at, at + CHUNK)
            fixed = got[rows, here] + jnp.dot(
                factor, right_split[:, here], preferred_element_type=jnp.float32
            )
            got[rows, here] = fixed
            square = fixed * fixed
            for lane in range(0, CHUNK, LANES):
                total = total + square[:, lane:lane + LANES]
            part = square[0:8]
            for n in range(8, height, 8):
                part = part + square[n:n + 8]
            col_sum[:, here] += part
        row_parts[q, pl.ds(slot, 1)] = jnp.sum(total.T, axis=0, keepdims=True)
        return carry

    lax.fori_loop(0, grid_rows * grid_cols, settle, 0)
    col_parts[p] = jnp.sum(col_sum[...], axis=0, keepdims=True)

    def row_part(n):
        dz, dc = n // 2, n % 2
        return copy(row_parts.at[q], row_parts.at[q], row_send.at[n], row_recv.at[n], target(0, dz, dc))

    def col_part(dp):
        return copy(col_parts.at[p], col_parts.at[p], col_send.at[dp], col_recv.at[dp], target(dp, 0, 0))

    for n in range(grid_cols - 1, 0, -1):
        row_part(n).start()
    for dp in range(1, grid_rows):
        col_part(dp).start()

    def drain(n, carry):
        tile(n // (2 * chips), n // 2 % chips, n % 2, 0, height).wait_send()
        return carry

    lax.fori_loop(1, grid_rows * grid_cols, drain, 0)
    for n in range(1, grid_cols):
        row_part(n).wait()
    for dp in range(1, grid_rows):
        col_part(dp).wait()


def exchange(covariance, left, right):
    grid_rows, grid_cols = lax.axis_size("prow"), lax.axis_size("pcol")
    everyone = grid_rows * grid_cols
    rows, breadth = covariance.shape
    rank = left.shape[0]
    height, width = rows // grid_rows, breadth // grid_cols
    dma = pltpu.SemaphoreType.DMA
    vmem = pl.BlockSpec(memory_space=pltpu.VMEM)
    hbm = pl.BlockSpec(memory_space=pltpu.HBM)
    return pl.pallas_call(
        functools.partial(exchange_kernel, grid_rows, grid_cols),
        out_shape=(
            pltpu.VMEM((everyone * height, width), jnp.float32),
            pltpu.VMEM((grid_cols, everyone, height), jnp.float32),
            pltpu.VMEM((grid_rows, 1, width), jnp.float32),
            pltpu.HBM((grid_rows, grid_cols, height, width), jnp.float32),
        ),
        in_specs=[hbm] * 3,
        out_specs=(vmem, vmem, vmem, hbm),
        scratch_shapes=[
            pltpu.VMEM((2, SLAB, breadth), jnp.float32),
            pltpu.VMEM((3, 2, grid_cols, SLAB, width), jnp.float32),
            pltpu.VMEM(left.shape, jnp.float32),
            pltpu.VMEM((grid_rows, rank, height), jnp.float32),
            pltpu.VMEM((2, grid_cols // 2, grid_rows, rank, height), jnp.float32),
            pltpu.VMEM((grid_rows,) + right.shape, jnp.float32),
            pltpu.VMEM((4 * rank, width), jnp.bfloat16),
            pltpu.VMEM((8, width), jnp.float32),
            dma((2,)), dma((3, 2)), dma((everyone,)), dma((everyone,)),
            dma((grid_rows,)), dma((grid_rows,)), dma((2,)), dma((grid_cols // 2,)),
            dma, dma, dma, dma, dma((grid_rows,)), dma((grid_rows,)), dma((4,)),
            dma((grid_cols,)), dma((grid_cols,)), dma((grid_rows,)), dma((grid_rows,)),
        ],
        compiler_params=pltpu.CompilerParams(
            collective_id=0, has_side_effects=True, vmem_limit_bytes=HELD * 1024 * 1024
        ),
    )(covariance, left, right)


def scale_kernel(order, got, row_parts, col_parts, out, stage, row_scale, sem):
    grid_cols, everyone, height = row_parts.shape
    width = got.shape[1]
    rows, cols = row_parts[0], col_parts[0]
    for n in range(1, grid_cols):
        rows = rows + row_parts[n]
    for n in range(1, col_parts.shape[0]):
        cols = cols + col_parts[n]
    row_scale[...] = lax.rsqrt(jnp.sqrt(rows / order + epsilon))
    col_scale = lax.rsqrt(jnp.sqrt(cols / order + epsilon))

    def store(n):
        return pltpu.make_async_copy(
            stage.at[n % STAGES], out.at[pl.ds(pl.multiple_of(n * height, height), height)], sem.at[n % STAGES]
        )

    def step(n, carry):
        @pl.when(n >= STAGES)
        def _():
            store(n - STAGES).wait()

        scale = jnp.broadcast_to(row_scale[pl.ds(n, 1)], (height, height)).T
        here = pl.ds(pl.multiple_of(n * height, height), height)
        for at in range(0, width, LANES):
            stage[n % STAGES, :, at:at + LANES] = got[here, at:at + LANES] * scale * col_scale[:, at:at + LANES]
        store(n).start()
        return carry

    lax.fori_loop(0, everyone, step, 0)
    for n in range(everyone - STAGES, everyone):
        store(n).wait()


def scaled(order, got, row_parts, col_parts):
    height, width = row_parts.shape[2], got.shape[1]
    vmem = pl.BlockSpec(memory_space=pltpu.VMEM)
    return pl.pallas_call(
        functools.partial(scale_kernel, order),
        out_shape=jax.ShapeDtypeStruct(got.shape, jnp.float32),
        in_specs=[vmem] * 3,
        out_specs=pl.BlockSpec(memory_space=pl.ANY),
        scratch_shapes=[
            pltpu.VMEM((STAGES, height, width), jnp.float32),
            pltpu.VMEM(row_parts.shape[1:], jnp.float32),
            pltpu.SemaphoreType.DMA((STAGES,)),
        ],
        compiler_params=pltpu.CompilerParams(vmem_limit_bytes=HELD * 1024 * 1024),
    )(got, row_parts, col_parts)


def direct_body(covariance, factor_left, factor_right):
    got, row_parts, col_parts, _ = exchange(covariance, factor_left, factor_right)
    held = [pltpu.with_memory_space_constraint(x, pltpu.VMEM) for x in (got, row_parts, col_parts)]
    return scaled(covariance.shape[1], *held)


def power_of_two(n):
    return n & (n - 1) == 0


def chosen(mesh, covariance):
    grid_rows, grid_cols = mesh.shape["prow"], mesh.shape["pcol"]
    tiles = covariance.shape[0] // (grid_rows * grid_cols * TILE)
    fits = tiles == 2 * grid_rows and grid_cols == 8
    across = covariance.shape[1] // (TILE * grid_cols)
    fits = fits and power_of_two(grid_rows) and grid_rows > 1 and across % 4 == 0
    return direct_body if fits else body


def solution(mesh):
    placed = (P(("prow", "pcol"), None), P(None, ("prow", "pcol")), P("prow", "pcol"))

    def run(covariance, factor_left, factor_right):
        return jax.shard_map(
            chosen(mesh, covariance), mesh=mesh, in_specs=placed, out_specs=P("prow", "pcol"), check_vma=False
        )(covariance, factor_left, factor_right)

    return run
```

```python
import functools

import jax
import jax.numpy as jnp
from jax import lax
from jax.experimental import pallas as pl
from jax.experimental.pallas import tpu as pltpu
from jax.sharding import PartitionSpec as P

ORDER = 16384
TILE = 64


epsilon = 1e-06


def deal_columns(source):
    height = source.shape[0]
    breadth = source.shape[1]
    grid_cols = lax.axis_size("pcol")
    arranged = (
        source.reshape(height, breadth // (TILE * grid_cols), grid_cols, TILE)
        .transpose(0, 2, 1, 3)
        .reshape(height, breadth)
    )
    return lax.all_to_all(arranged, "pcol", split_axis=1, concat_axis=0, tiled=True)


def order_rows(source):
    height = source.shape[0]
    breadth = source.shape[1]
    grid_rows = lax.axis_size("prow")
    grouped = source.reshape(height // (TILE * grid_rows), grid_rows, TILE, breadth)
    return grouped.transpose(1, 0, 2, 3).reshape(height, breadth)


def body(covariance, factor_left, factor_right):
    right_panel = lax.all_gather(factor_right, "prow", axis=0, tiled=True)
    dealt = deal_columns(covariance)
    left_block = lax.all_gather(factor_left, "pcol", axis=1, tiled=True).T
    tiles_moved, left_rows = (
        lax.all_to_all(order_rows(dealt), "prow", split_axis=0, concat_axis=0, tiled=True),
        lax.all_to_all(order_rows(left_block), "prow", split_axis=0, concat_axis=0, tiled=True),
    )
    corrected = tiles_moved + jnp.dot(
        left_rows, right_panel, precision=lax.Precision.HIGHEST, preferred_element_type=jnp.float32
    )
    squared = corrected * corrected
    row_total = lax.psum(jnp.sum(squared, axis=1), "pcol")
    col_total = lax.psum(jnp.sum(squared, axis=0), "prow")
    row_mean = row_total / ORDER + epsilon
    col_mean = col_total / ORDER + epsilon
    return corrected * lax.rsqrt(jnp.sqrt(row_mean[:, None] * col_mean[None, :]))


def flip(index, size, bits):
    out, unit = 0, 1
    while unit < size:
        out = out + unit * ((index // unit + bits // unit) % 2)
        unit *= 2
    return out


SLAB = TILE // 2
LANES = 128
CHUNK = 256
STAGES = 4
HELD = 26


def deal_slab(grid_cols, src, dst):
    low = lax.broadcasted_iota(jnp.int32, (src.shape[0], LANES), 1) < TILE
    for pair in range(grid_cols // 2):
        for m in range(src.shape[1] // (LANES * grid_cols)):
            at = (pair + grid_cols * m) * LANES
            first = src[:, at:at + LANES]
            at += grid_cols // 2 * LANES
            second = src[:, at:at + LANES]
            dst[2 * pair, :, m * LANES:(m + 1) * LANES] = jnp.where(low, first, pltpu.roll(second, TILE, 1))
            dst[2 * pair + 1, :, m * LANES:(m + 1) * LANES] = jnp.where(low, pltpu.roll(first, TILE, 1), second)


def exchange_kernel(
    grid_rows, grid_cols,
    cov, left, right, got, row_parts, col_parts, tiles,
    slab_in, slab_out, left_in, left_own, lefts, rights, right_split, col_sum,
    in_sem, out_sem, tile_send, tile_recv, plane_send, plane_recv, block_send, block_recv,
    relay_send, relay_recv, swap_send, swap_recv, right_send, right_recv, own_sem,
    row_send, row_recv, col_send, col_recv,
):
    chips = grid_cols // 2
    p, q = lax.axis_index("prow"), lax.axis_index("pcol")
    z, core = q // 2, q % 2
    height = tiles.shape[2]
    rank = left.shape[0]
    beside = (z + z // 2) % 2
    half = z // 2
    mate = flip(z, chips, 1)
    far = jnp.maximum(z, 3 - z)

    def copy(src, dst, send, recv, to):
        return pltpu.make_async_remote_copy(
            src_ref=src, dst_ref=dst, send_sem=send, recv_sem=recv,
            device_id=to, device_id_type=pl.DeviceIdType.MESH,
        )

    def target(dp, dz, dc):
        return flip(p, grid_rows, dp), 2 * flip(z, chips, dz) + (core + dc) % 2

    def slab_load(t, h):
        at = ((t % 2) * grid_rows + flip(p, grid_rows, t // 2)) * TILE + h * SLAB
        return pltpu.make_async_copy(cov.at[pl.ds(pl.multiple_of(at, SLAB), SLAB)], slab_in.at[h], in_sem.at[h])

    def slab_slot(t):
        return jnp.where(t == 0, 2, t % 2)

    def slab_store(t, h):
        at = (t % 2) * TILE + h * SLAB
        return pltpu.make_async_copy(
            slab_out.at[slab_slot(t), h],
            tiles.at[flip(p, grid_rows, t // 2), :, pl.ds(pl.multiple_of(at, SLAB), SLAB)],
            out_sem.at[slab_slot(t), h],
        )

    for h in range(2):
        slab_load(0, h).start()
    load_left = pltpu.make_async_copy(left, left_in, own_sem.at[3])
    load_left.start()

    barrier = pltpu.get_barrier_semaphore()
    for dp in range(grid_rows):
        for dz in range(chips):
            for dc in range(2):
                if (dp, dz, dc) != (0, 0, 0):
                    pl.semaphore_signal(
                        barrier, inc=1, device_id=target(dp, dz, dc), device_id_type=pl.DeviceIdType.MESH
                    )

    def pick_left():
        low = lax.broadcasted_iota(jnp.int32, (rank, LANES), 1) < TILE
        for to in range(grid_rows):
            at = to // 2 * LANES
            first = left_in[:, at:at + LANES]
            at += grid_rows * TILE
            second = left_in[:, at:at + LANES]
            if to % 2 == 0:
                left_own[to] = jnp.where(low, first, pltpu.roll(second, TILE, 1))
            else:
                left_own[to] = jnp.where(low, pltpu.roll(first, TILE, 1), second)

    def plane(dp):
        return copy(
            left_own.at[flip(p, grid_rows, dp)], lefts.at[core, z, p],
            plane_send.at[dp], plane_recv.at[dp], target(dp, 0, 0),
        )

    def beside_right(dp):
        return copy(right, rights.at[p], right_send.at[dp], right_recv.at[dp], target(dp, 0, 0))

    keep_left = pltpu.make_async_copy(left_own.at[p], lefts.at[core, z, p], own_sem.at[0])
    keep_right = pltpu.make_async_copy(right, rights.at[p], own_sem.at[1])

    block = lefts.at[core, z]
    gate = 2 - half
    to_mate = copy(block, block, block_send.at[0], block_recv.at[z], (p, 2 * mate + core))
    to_gate = copy(block, block, block_send.at[1], block_recv.at[z], (p, 2 * gate + core))
    other = lefts.at[core, pl.ds(2 * (1 - half), 2)]
    relay = copy(other, other, relay_send, relay_recv, (p, 2 * mate + core))
    swap = copy(lefts.at[core], lefts.at[core], swap_send, swap_recv, target(0, 0, 1))
    own_rows = pl.ds(pl.multiple_of((p * grid_cols + q) * height, height), height)
    keep_tiles = pltpu.make_async_copy(tiles.at[p, q], got.at[own_rows], own_sem.at[2])

    def tile(dp, dz, dc, start, count):
        to = target(dp, dz, dc)
        at = pl.multiple_of((p * grid_cols + q) * height + start, TILE)
        n = (dp * chips + dz) * 2 + dc
        return copy(
            tiles.at[to[0], to[1], pl.ds(start, count)], got.at[pl.ds(at, count)], tile_send.at[n], tile_recv.at[n], to
        )

    def send_slab(h):
        at = pl.multiple_of((p * grid_cols + q) * height + h * SLAB, SLAB)
        for i in range(2):
            dz = beside * (3 - i) + (1 - beside) * (1 - i)
            for dc in range(2):
                to = target(0, dz, dc)
                n = dz * 2 + dc

                @pl.when(dz + dc != 0)
                def _():
                    copy(
                        slab_out.at[2, h, to[1]], got.at[pl.ds(at, SLAB)], tile_send.at[n], tile_recv.at[n], to
                    ).start()

    def send_tiles(dp, kind, start=0):
        for i in range(2):
            dz = kind * (3 - i) + (1 - kind) * (1 - i)
            for dc in range(2):

                @pl.when(dp + dz + dc != 0)
                def _():
                    tile(dp, dz, dc, start, height - start).start()

    def deal(t, carry):
        @pl.when(t < 2 * grid_rows)
        def _():
            for h in range(2):
                slab_load(t, h).wait()
                deal_slab(grid_cols, slab_in.at[h], slab_out.at[slab_slot(t), h])

                @pl.when(t + 1 < 2 * grid_rows)
                def _():
                    slab_load(t + 1, h).start()

                slab_store(t, h).start()

                @pl.when((t == 0) & (h == 0))
                def _():
                    pl.semaphore_wait(barrier, grid_rows * grid_cols - 1)
                    send_slab(0)
                    load_left.wait()
                    pick_left()
                    keep_right.start()
                    for dp in range(1, grid_rows):
                        beside_right(dp).start()

                @pl.when((t == 0) & (h == 1))
                def _():
                    send_slab(1)
                    keep_left.start()
                    for dp in range(1, grid_rows):
                        plane(dp).start()

        @pl.when(t > 0)
        def _():
            for h in range(2):
                slab_store(t - 1, h).wait()

        @pl.when(t == 2)
        def _():
            send_tiles(0, beside, TILE)

        @pl.when(t == 1)
        def _():
            keep_left.wait()
            for dp in range(1, grid_rows):
                plane(dp).wait()
            to_gate.start()
            to_mate.start()

        @pl.when((t > 2) & (t % 2 == 0))
        def _():
            send_tiles(t // 2 - 1, beside)
            send_tiles(t // 2 - 2, 1 - beside)

        return carry

    lax.fori_loop(0, 2 * grid_rows + 1, deal, 0)
    keep_tiles.start()

    to_gate.wait_send()
    to_mate.wait_send()

    def arrived(which):
        there = lefts.at[core, which]
        return copy(there, there, block_send.at[0], block_recv.at[which], (p, 2 * mate + core))

    arrived(mate).wait_recv()

    @pl.when(beside == 1)
    def _():
        for i in range(2):
            arrived(2 * (1 - half) + i).wait_recv()
        relay.start()

    send_tiles(grid_rows - 1, 1 - beside)
    keep_right.wait()
    for dp in range(1, grid_rows):
        beside_right(dp).wait()
    depth = right.shape[0]
    for n in range(grid_rows):
        value = rights[n]
        high = value.astype(jnp.bfloat16)
        rest = (value - high.astype(jnp.float32)).astype(jnp.bfloat16)
        right_split[n * depth:(n + 1) * depth] = high
        right_split[rank + n * depth:rank + (n + 1) * depth] = rest
        right_split[2 * rank + n * depth:2 * rank + (n + 1) * depth] = high
        right_split[3 * rank + n * depth:3 * rank + (n + 1) * depth] = rest
    col_sum[...] = jnp.zeros_like(col_sum)

    @pl.when(beside == 0)
    def _():
        relay.wait_recv()

    @pl.when(beside == 1)
    def _():
        relay.wait_send()

    swap.start()
    swap.wait()
    keep_tiles.wait()

    width = got.shape[1]

    def settle(m, carry):
        group = m // (2 * grid_rows)
        dz = jnp.where(group == 3, 5 - far, jnp.where(group == 2, far, group))
        dp, dc = m % (2 * grid_rows) // 2, m % 2
        from_p, from_q = target(dp, dz, dc)
        slot = from_p * grid_cols + from_q

        @pl.when(dp + dz + dc != 0)
        def _():
            n = (dp * chips + dz) * 2 + dc
            there = got.at[pl.ds(pl.multiple_of(slot * height, height), height)]
            copy(tiles.at[0, 0], there, tile_send.at[n], tile_recv.at[n], (from_p, from_q)).wait_recv()

        value = lefts[from_q % 2, from_q // 2, from_p]
        high = value.astype(jnp.bfloat16).astype(jnp.float32)
        stack = jnp.concatenate([high, high, value - high, value - high], axis=0)
        factor = stack.T.astype(jnp.bfloat16)
        rows = pl.ds(pl.multiple_of(slot * height, height), height)
        total = jnp.zeros((height, LANES), jnp.float32)
        for at in range(0, width, CHUNK):
            here = slice(at, at + CHUNK)
            fixed = got[rows, here] + jnp.dot(
                factor, right_split[:, here], preferred_element_type=jnp.float32
            )
            got[rows, here] = fixed
            square = fixed * fixed
            for lane in range(0, CHUNK, LANES):
                total = total + square[:, lane:lane + LANES]
            part = square[0:8]
            for n in range(8, height, 8):
                part = part + square[n:n + 8]
            col_sum[:, here] += part
        row_parts[q, pl.ds(slot, 1)] = jnp.sum(total.T, axis=0, keepdims=True)
        return carry

    lax.fori_loop(0, grid_rows * grid_cols, settle, 0)
    col_parts[p] = jnp.sum(col_sum[...], axis=0, keepdims=True)

    def row_part(n):
        dz, dc = n // 2, n % 2
        return copy(row_parts.at[q], row_parts.at[q], row_send.at[n], row_recv.at[n], target(0, dz, dc))

    def col_part(dp):
        return copy(col_parts.at[p], col_parts.at[p], col_send.at[dp], col_recv.at[dp], target(dp, 0, 0))

    for n in range(grid_cols - 1, 0, -1):
        row_part(n).start()
    for dp in range(1, grid_rows):
        col_part(dp).start()

    def drain(n, carry):
        tile(n // (2 * chips), n // 2 % chips, n % 2, 0, height).wait_send()
        return carry

    lax.fori_loop(1, grid_rows * grid_cols, drain, 0)
    for n in range(1, grid_cols):
        row_part(n).wait()
    for dp in range(1, grid_rows):
        col_part(dp).wait()


def exchange(covariance, left, right):
    grid_rows, grid_cols = lax.axis_size("prow"), lax.axis_size("pcol")
    everyone = grid_rows * grid_cols
    rows, breadth = covariance.shape
    rank = left.shape[0]
    height, width = rows // grid_rows, breadth // grid_cols
    dma = pltpu.SemaphoreType.DMA
    vmem = pl.BlockSpec(memory_space=pltpu.VMEM)
    hbm = pl.BlockSpec(memory_space=pltpu.HBM)
    return pl.pallas_call(
        functools.partial(exchange_kernel, grid_rows, grid_cols),
        out_shape=(
            pltpu.VMEM((everyone * height, width), jnp.float32),
            pltpu.VMEM((grid_cols, everyone, height), jnp.float32),
            pltpu.VMEM((grid_rows, 1, width), jnp.float32),
            pltpu.HBM((grid_rows, grid_cols, height, width), jnp.float32),
        ),
        in_specs=[hbm] * 3,
        out_specs=(vmem, vmem, vmem, hbm),
        scratch_shapes=[
            pltpu.VMEM((2, SLAB, breadth), jnp.float32),
            pltpu.VMEM((3, 2, grid_cols, SLAB, width), jnp.float32),
            pltpu.VMEM(left.shape, jnp.float32),
            pltpu.VMEM((grid_rows, rank, height), jnp.float32),
            pltpu.VMEM((2, grid_cols // 2, grid_rows, rank, height), jnp.float32),
            pltpu.VMEM((grid_rows,) + right.shape, jnp.float32),
            pltpu.VMEM((4 * rank, width), jnp.bfloat16),
            pltpu.VMEM((8, width), jnp.float32),
            dma((2,)), dma((3, 2)), dma((everyone,)), dma((everyone,)),
            dma((grid_rows,)), dma((grid_rows,)), dma((2,)), dma((grid_cols // 2,)),
            dma, dma, dma, dma, dma((grid_rows,)), dma((grid_rows,)), dma((4,)),
            dma((grid_cols,)), dma((grid_cols,)), dma((grid_rows,)), dma((grid_rows,)),
        ],
        compiler_params=pltpu.CompilerParams(
            collective_id=0, has_side_effects=True, vmem_limit_bytes=HELD * 1024 * 1024
        ),
    )(covariance, left, right)


def scale_kernel(order, got, row_parts, col_parts, out, stage, row_scale, sem):
    grid_cols, everyone, height = row_parts.shape
    width = got.shape[1]
    rows, cols = row_parts[0], col_parts[0]
    for n in range(1, grid_cols):
        rows = rows + row_parts[n]
    for n in range(1, col_parts.shape[0]):
        cols = cols + col_parts[n]
    row_scale[...] = lax.rsqrt(jnp.sqrt(rows / order + epsilon))
    col_scale = lax.rsqrt(jnp.sqrt(cols / order + epsilon))

    def store(n):
        return pltpu.make_async_copy(
            stage.at[n % STAGES], out.at[pl.ds(pl.multiple_of(n * height, height), height)], sem.at[n % STAGES]
        )

    def step(n, carry):
        @pl.when(n >= STAGES)
        def _():
            store(n - STAGES).wait()

        scale = jnp.broadcast_to(row_scale[pl.ds(n, 1)], (height, height)).T
        here = pl.ds(pl.multiple_of(n * height, height), height)
        for at in range(0, width, LANES):
            stage[n % STAGES, :, at:at + LANES] = got[here, at:at + LANES] * scale * col_scale[:, at:at + LANES]
        store(n).start()
        return carry

    lax.fori_loop(0, everyone, step, 0)
    for n in range(everyone - STAGES, everyone):
        store(n).wait()


def scaled(order, got, row_parts, col_parts):
    height, width = row_parts.shape[2], got.shape[1]
    vmem = pl.BlockSpec(memory_space=pltpu.VMEM)
    return pl.pallas_call(
        functools.partial(scale_kernel, order),
        out_shape=jax.ShapeDtypeStruct(got.shape, jnp.float32),
        in_specs=[vmem] * 3,
        out_specs=pl.BlockSpec(memory_space=pl.ANY),
        scratch_shapes=[
            pltpu.VMEM((STAGES, height, width), jnp.float32),
            pltpu.VMEM(row_parts.shape[1:], jnp.float32),
            pltpu.SemaphoreType.DMA((STAGES,)),
        ],
        compiler_params=pltpu.CompilerParams(vmem_limit_bytes=HELD * 1024 * 1024),
    )(got, row_parts, col_parts)


def direct_body(covariance, factor_left, factor_right):
    got, row_parts, col_parts, _ = exchange(covariance, factor_left, factor_right)
    held = [pltpu.with_memory_space_constraint(x, pltpu.VMEM) for x in (got, row_parts, col_parts)]
    return scaled(covariance.shape[1], *held)


def power_of_two(n):
    return n & (n - 1) == 0


def chosen(mesh, covariance):
    grid_rows, grid_cols = mesh.shape["prow"], mesh.shape["pcol"]
    tiles = covariance.shape[0] // (grid_rows * grid_cols * TILE)
    fits = tiles == 2 * grid_rows and grid_cols == 8
    across = covariance.shape[1] // (TILE * grid_cols)
    fits = fits and power_of_two(grid_rows) and grid_rows > 1 and across % 4 == 0
    return direct_body if fits else body


def solution(mesh):
    placed = (P(("prow", "pcol"), None), P(None, ("prow", "pcol")), P("prow", "pcol"))

    def run(covariance, factor_left, factor_right):
        return jax.shard_map(
            chosen(mesh, covariance), mesh=mesh, in_specs=placed, out_specs=P("prow", "pcol"), check_vma=False
        )(covariance, factor_left, factor_right)

    return run
```
